256 devices in a mesh: groups: 4 (over x, y), seq: 64 (over z, core).
Axes of the slice: x: 2, y: 2, z: 32, core: 2. Of those that a mesh axis runs over, the one named last changes fastest.
The devices are a block of a 4x8x32 slice.
Arguments:
- queries: bfloat16 [32768, 1792], P(('groups', 'seq')), parts along dimension 0, may hold values from -100 to 100
- key_rows: bfloat16 [32768, 256], P(('groups', 'seq')), parts along dimension 0, may hold values from -100 to 100
- value_rows: bfloat16 [32768, 256], P(('groups', 'seq')), parts along dimension 0, may hold values from -6 to 6
- span_order: int32 [512], P('groups'), parts along dimension 0, may hold values from 0 to 127, each once
- kept_blocks: int32 [8, 4], P('groups'), parts along dimension 0, may hold values from 0 to 15, as said below
Outputs:
- attended: bfloat16 [32768, 1792], P(('groups', 'seq')), parts along dimension 0
- kept_cache: bfloat16 [8192, 512], P(('groups', 'seq')), parts along dimension 0
The draws below stay inside these ranges and needn't reach their ends.
There are 4 independent parts, one for each index of `groups`. The reference program is written for one: setup_inputs(seed, part) draws one part's arguments, and reference() takes and returns one part's arrays. A program takes and returns all parts, laid end to end along the dimension named above; each array names one. Nothing has to cross between parts.
Inputs may be any that keep to these rules, and one draw needn't show every extreme that they name: `kept_blocks`: each row lists 4 different blocks.
All inputs are finite; a program needn't handle non-finite values.
Results may differ from the reference program's by a relative error of at most 0.0055.
Values may be sent and summed in bfloat16 or wider, within the bound.
No kernel may reach another device: no remote copies, remote signals or barrier semaphores. Data moves between devices by JAX's collectives and lax.ppermute only.
A program may use at most 64 MiB of HBM per device.

```python
import math
import jax
import jax.numpy as jnp
from jax import lax

HEAD_DIM = 128
Q_HEADS = 14
KV_HEADS = 2
GROUP = 7
TOK_DEV = 128
TOKENS = 8192
SPANS = 128
BLOCK = 512
NBLOCKS = 16
KEEP = 4
CACHE_ROWS = 2048


def joint_draw(key):
    key_query = jax.random.fold_in(key, 101)
    key_keys = jax.random.fold_in(key, 102)
    query_part = jnp.clip(jax.random.normal(key_query, (TOKENS, KV_HEADS, GROUP, HEAD_DIM)), -6.0, 6.0)
    key_part = jnp.clip(jax.random.normal(key_keys, (TOKENS, KV_HEADS, HEAD_DIM)), -6.0, 6.0)
    return (query_part.reshape(TOKENS, Q_HEADS * HEAD_DIM), key_part.reshape(TOKENS, KV_HEADS * HEAD_DIM))


def draw_queries(key, part):
    query_part, key_part = joint_draw(key)
    return query_part.astype(jnp.bfloat16)


def draw_key_rows(key, part):
    query_part, key_part = joint_draw(key)
    return key_part.astype(jnp.bfloat16)


def draw_kept_blocks(key, part):
    shuffled = jax.random.permutation(jax.random.fold_in(key, 300), NBLOCKS).astype(jnp.int32)
    picks = (jnp.arange(KV_HEADS, dtype=jnp.int32)[:, None] * KEEP + jnp.arange(KEEP, dtype=jnp.int32)[None, :]) % NBLOCKS
    return shuffled[picks].astype(jnp.int32)


def block_scale(key, dims, cuts, smallest, top_value):
    factor_of, own = 1.0, jax.random.fold_in(key, 6)
    for position, parts in cuts:
        draws = jnp.exp(jax.random.uniform(jax.random.fold_in(own, position), (parts,), jnp.float32, smallest / len(cuts), top_value / len(cuts)))
        factor_of = factor_of * jnp.repeat(draws, dims[position] // parts).reshape([-1 if axis == position else 1 for axis in range(len(dims))])
    return factor_of


def bell_draw(own_key, extent, width, reach, split=(), kind=jnp.bfloat16):
    entries = width * jax.random.normal(own_key, extent, jnp.float32)
    if split:
        entries = entries * block_scale(own_key, extent, split, -0.22, 0.18)
    return jnp.clip(entries, -reach, reach).astype(kind)


def setup_inputs(seed: int = 0, part: int = 0) -> dict:
    splits = jax.random.split(jax.random.key(seed), 6)
    part_keys = jax.random.split(jax.random.fold_in(splits[5], part), 6)
    return {
        "queries": draw_queries(jax.random.fold_in(jax.random.fold_in(splits[5], part), 71), part),
        "key_rows": draw_key_rows(jax.random.fold_in(jax.random.fold_in(splits[5], part), 71), part),
        "value_rows": bell_draw(part_keys[2], (TOKENS, KV_HEADS * HEAD_DIM), 1.0, 6.0, ((0, 64),)),
        "span_order": jax.random.permutation(part_keys[3], SPANS).astype(jnp.int32),
        "kept_blocks": draw_kept_blocks(jax.random.fold_in(jax.random.fold_in(splits[5], part), 71), part),
    }


def token_positions(span_order, span_len):
    within = jnp.arange(span_len, dtype=jnp.int32)
    return (span_order.astype(jnp.int32)[:, None] * span_len + within[None, :]).reshape(-1).astype(jnp.int32)

def cache_sources(kept_blocks, row_ids):
    block_ids = row_ids // BLOCK
    match = jnp.arange(kept_blocks.shape[1], dtype=jnp.int32)[None, None, :] == block_ids[None, :, None]
    chosen = lax.optimization_barrier(jnp.sum(jnp.where(match, kept_blocks.astype(jnp.int32)[:, None, :], 0), axis=-1))
    return (chosen * BLOCK + row_ids[None, :] % BLOCK).astype(jnp.int32)

def reference(queries, key_rows, value_rows, span_order, kept_blocks):
    positions = token_positions(span_order, TOK_DEV // 2)
    scale = 1.0 / math.sqrt(HEAD_DIM)
    query_heads = queries.reshape(TOKENS, KV_HEADS, GROUP, HEAD_DIM)
    key_heads = key_rows.reshape(TOKENS, KV_HEADS, HEAD_DIM)
    value_heads = value_rows.reshape(TOKENS, KV_HEADS, HEAD_DIM)
    query_block = math.gcd(TOKENS, 512)
    query_blocks = TOKENS // query_block

    def one_block(index):
        index = index.astype(jnp.int32)
        head_index = (index // query_blocks).astype(jnp.int32)
        row_start = (index % query_blocks * query_block).astype(jnp.int32)
        zero_index = jnp.zeros((), jnp.int32)
        block_queries = lax.dynamic_slice(query_heads, (row_start, head_index, zero_index, zero_index), (query_block, 1, GROUP, HEAD_DIM))[:, 0]
        head_keys = lax.dynamic_index_in_dim(key_heads, head_index, 1, keepdims=False)
        head_values = lax.dynamic_index_in_dim(value_heads, head_index, 1, keepdims=False)
        block_pos = lax.dynamic_slice_in_dim(positions, row_start, query_block)
        scores = jnp.einsum('qgd,kd->gqk', block_queries.astype(jnp.float32), head_keys.astype(jnp.float32)) * scale
        visible = positions[None, None, :] <= block_pos[None, :, None]
        scores = jnp.where(visible, scores, -1e+30)
        row_max = lax.optimization_barrier(jnp.max(scores, axis=-1))
        weights = jnp.where(visible, jnp.exp(scores - row_max[..., None]), 0.0)
        totals = lax.optimization_barrier(jnp.sum(weights, axis=-1))
        rounded = weights.astype(jnp.bfloat16)
        mixed = jnp.einsum('gqk,kd->gqd', rounded.astype(jnp.float32), head_values.astype(jnp.float32)) / totals[..., None]
        return jnp.transpose(mixed, (1, 0, 2)).astype(jnp.bfloat16)
    results = lax.map(one_block, jnp.arange(KV_HEADS * query_blocks, dtype=jnp.int32))
    attended = results.reshape(KV_HEADS, query_blocks, query_block, GROUP, HEAD_DIM)
    attended = jnp.transpose(attended, (1, 2, 0, 3, 4)).reshape(TOKENS, Q_HEADS * HEAD_DIM)
    natural = jnp.zeros((TOKENS, 2 * KV_HEADS * HEAD_DIM), jnp.bfloat16)
    natural = natural.at[positions].set(jnp.concatenate([key_rows, value_rows], axis=1))
    sources = cache_sources(kept_blocks, jnp.arange(CACHE_ROWS, dtype=jnp.int32))
    columns = []
    for part_index in range(2):
        for head_index in range(KV_HEADS):
            low_col = part_index * KV_HEADS * HEAD_DIM + head_index * HEAD_DIM
            columns.append(natural[sources[head_index], low_col:low_col + HEAD_DIM])
    kept_cache = jnp.concatenate(columns, axis=1)
    return (attended, kept_cache)
```

```python
import functools
import math

import jax
import jax.numpy as jnp
from jax import lax
from jax.experimental import pallas as pl
from jax.experimental.pallas import tpu as pltpu
from jax.sharding import PartitionSpec as P


HEAD_DIM = 128
BLOCK = 512
LOW = -1e20
HIDDEN = -1e30
UNROLL = 7
SETUP_VMEM = 63 * 2**20
VMEM = pl.BlockSpec(memory_space=pltpu.VMEM)
SMEM = pl.BlockSpec(memory_space=pltpu.SMEM)


def attend_kernel(first, kv_heads, group, row, count, qo_ref, qp_ref, kpos_ref, qpos_ref, *refs):
    pieces, refs = refs[:count], refs[count:]
    if first:
        m_out, l_out, acc_out, bias, keys, values = refs
        m_in = l_in = acc_in = None
    else:
        m_in, l_in, acc_in, m_out, l_out, acc_out, bias, keys, values = refs
    rows = qo_ref.shape[0]
    piece = pieces[0].shape[0]
    scale = math.log2(math.e) / math.sqrt(HEAD_DIM)
    ones = jnp.ones((count * piece, HEAD_DIM), jnp.bfloat16)
    for n, ref in enumerate(pieces):
        part = slice(n * piece, (n + 1) * piece)
        kpos = kpos_ref[row + n // 2 : row + n // 2 + 1, (n % 2) * piece : (n % 2 + 1) * piece]
        bias[:, part] = jnp.where(kpos <= qpos_ref[...], 0.0, HIDDEN)
        for h in range(kv_heads):
            keys[h, part, :] = ref[:, h * HEAD_DIM : (h + 1) * HEAD_DIM]
            values[h, part, 0:HEAD_DIM] = ref[:, (kv_heads + h) * HEAD_DIM : (kv_heads + h + 1) * HEAD_DIM]
    for h in range(kv_heads):
        values[h, :, HEAD_DIM:] = ones

    def one_head(j):
        h = j // group
        at = pl.ds(pl.multiple_of(j * HEAD_DIM, HEAD_DIM), HEAD_DIM)
        q = jnp.concatenate([qo_ref[:, at], qp_ref[:, at]], axis=0)
        s = lax.dot_general(q, keys[h], (((1,), (1,)), ((), ())), preferred_element_type=jnp.float32)
        s = s + bias[...]
        top = jnp.max(s, axis=1, keepdims=True)
        if first:
            m_new = jnp.broadcast_to(jnp.maximum(top, LOW), (2 * rows, HEAD_DIM))
        else:
            m_old = m_in[:, at]
            m_new = jnp.maximum(m_old, top)
        shift = m_new * scale
        weights = jnp.exp2(s * scale - jnp.concatenate([shift] * count, axis=1)).astype(jnp.bfloat16)
        mixed = jnp.dot(weights, values[h], preferred_element_type=jnp.float32)
        m_out[:, at] = m_new
        if first:
            acc_out[:, at] = mixed[:, :HEAD_DIM]
            l_out[:, at] = mixed[:, HEAD_DIM:]
        else:
            factor = jnp.exp2((m_old - m_new) * scale)
            acc_out[:, at] = acc_in[:, at] * factor + mixed[:, :HEAD_DIM]
            l_out[:, at] = l_in[:, at] * factor + mixed[:, HEAD_DIM:]

    def some_heads(step, carry):
        for u in range(UNROLL):
            one_head(step * UNROLL + u)
        return carry

    lax.fori_loop(0, kv_heads * group // UNROLL, some_heads, 0)


def attend(row, kv_heads, group, qo, qp, pieces, kpos, qpos, state):
    rows, width = qo.shape
    count, piece = len(pieces), pieces[0].shape[0]
    part = jax.ShapeDtypeStruct((2 * rows, width), jnp.float32)
    first = state is None
    args = (qo, qp, kpos, qpos) + tuple(pieces) + (() if first else tuple(state))
    flops = 2 * 2 * 2 * rows * count * piece * width * 2
    return pl.pallas_call(
        functools.partial(attend_kernel, first, kv_heads, group, row, count),
        out_shape=(part, part, part),
        in_specs=[VMEM] * len(args),
        out_specs=(VMEM,) * 3,
        scratch_shapes=[
            pltpu.VMEM((2 * rows, count * piece), jnp.float32),
            pltpu.VMEM((kv_heads, count * piece, HEAD_DIM), jnp.bfloat16),
            pltpu.VMEM((kv_heads, count * piece, 2 * HEAD_DIM), jnp.bfloat16),
        ],
        input_output_aliases={} if first else {4 + count + i: i for i in range(3)},
        compiler_params=pltpu.CompilerParams(vmem_limit_bytes=8 * 2**20),
        cost_estimate=pl.CostEstimate(flops=flops, bytes_accessed=2**20, transcendentals=2**20),
        name="attend",
    )(*args)


def moves_right(core, r):
    return lax.rem(core + r, 2)


def setup_kernel(kv_heads, chips, span, cache_rows, me_ref, order_hbm, row_hbm, kept_hbm, k_hbm, v_hbm, own_ref, kpos_ref, qpos_ref, meta_ref, order_ref, row_ref, kept_ref, sems):
    width = k_hbm.shape[1]
    copies = [
        pltpu.make_async_copy(order_hbm, order_ref, sems.at[0]),
        pltpu.make_async_copy(row_hbm, row_ref, sems.at[1]),
        pltpu.make_async_copy(kept_hbm, kept_ref, sems.at[2]),
        pltpu.make_async_copy(k_hbm, own_ref.at[:, :width], sems.at[3]),
        pltpu.make_async_copy(v_hbm, own_ref.at[:, width:], sems.at[4]),
    ]
    for copy in copies:
        copy.start()
    me = me_ref[0]
    chip, core = me // 2, lax.rem(me, 2)
    half = chips // 2
    lane = lax.broadcasted_iota(jnp.int32, (1, 4 * span), 1)
    row = lax.broadcasted_iota(jnp.int32, (4 * span, HEAD_DIM), 0)
    for copy in copies[:3]:
        copy.wait()
    for s in range(half + 1):
        r = (s - 1) // 2
        from_chip = chip if s == 0 else lax.rem(chip + s - 2 * s * moves_right(core, r) + chips, chips)
        first = core if s == 0 or r % 2 == 1 else 1 - core
        src = (2 * from_chip + first, 2 * from_chip + 1 - first)
        spans = [order_ref[2 * d + i] for d in src for i in range(2)]
        kpos = lane + spans[0] * span
        for i in range(1, 4):
            kpos = jnp.where(lane >= i * span, lane + (spans[i] - i) * span, kpos)
        if s == 0:
            kpos = kpos + core * 2**30
            qpos = row + spans[0] * span
            for i in range(1, 4):
                qpos = jnp.where(row >= i * span, row + (spans[i] - i) * span, qpos)
            qpos_ref[...] = qpos
        if s == half:
            kpos = kpos + (1 - moves_right(core, r)) * 2**30
        kpos_ref[s : s + 1, :] = kpos
    slots = lax.broadcasted_iota(jnp.int32, row_ref.shape, 1)
    for o in range(2):
        owner = me + o * (1 - 2 * core)
        first_row = owner * cache_rows
        for h in range(kv_heads):
            src = kept_ref[h, first_row // BLOCK] * BLOCK + lax.rem(first_row, BLOCK)
            slot = jnp.sum(jnp.where(row_ref[...] == src // span, slots, 0))
            dev = slot // 2
            back = lax.rem(chip - dev // 2 + chips, chips)
            right = jnp.where(back <= half, 1, 0)
            far = jnp.where(back <= half, back, chips - back)
            r = (far + 1) // 2 - 1
            here = jnp.where(far == 0, core == 0, moves_right(core, r + 2) == right)
            same = (far == 0) | (lax.rem(r + 2, 2) == 1)
            first = jnp.where(same, core, 1 - core)
            side = jnp.where(lax.rem(dev, 2) == first, 0, 1)
            at = (o * kv_heads + h) * 2
            meta_ref[at] = jnp.where(here, 2 * far + side, -1)
            meta_ref[at + 1] = lax.rem(slot, 2) * span + lax.rem(src, span)
    for copy in copies[3:]:
        copy.wait()


def setup(kv_heads, chips, cache_rows, me, span_order, kept_blocks, key_rows, value_rows):
    rows, width = key_rows.shape
    rounds = -(-(chips // 2 + 1) // 8) * 8
    return pl.pallas_call(
        functools.partial(setup_kernel, kv_heads, chips, rows // 2, cache_rows),
        out_shape=(
            jax.ShapeDtypeStruct((rows, 2 * width), jnp.bfloat16),
            jax.ShapeDtypeStruct((rounds, 2 * rows), jnp.int32),
            jax.ShapeDtypeStruct((2 * rows, HEAD_DIM), jnp.int32),
            jax.ShapeDtypeStruct((4 * kv_heads,), jnp.int32),
        ),
        in_specs=[SMEM] + [pl.BlockSpec(memory_space=pltpu.HBM)] * 5,
        out_specs=(VMEM, VMEM, VMEM, SMEM),
        scratch_shapes=[
            pltpu.SMEM(span_order.shape, jnp.int32),
            pltpu.VMEM((1,) + span_order.shape, jnp.int32),
            pltpu.SMEM(kept_blocks.shape, jnp.int32),
            pltpu.SemaphoreType.DMA((5,)),
        ],
        compiler_params=pltpu.CompilerParams(vmem_limit_bytes=SETUP_VMEM),
        name="setup",
    )(me.reshape(1), span_order, span_order.reshape(1, -1), kept_blocks, key_rows, value_rows)


def pick_kernel(kv_heads, pieces, meta_ref, *refs):
    ins, out_ref = refs[: len(pieces)], refs[len(pieces)]
    out_ref[...] = jnp.zeros_like(out_ref)
    owners = 2
    rows = out_ref.shape[1]
    for o in range(owners):
        for h in range(kv_heads):
            at = (o * kv_heads + h) * 2
            piece = meta_ref[at]
            start = pl.multiple_of(meta_ref[at + 1], 32)
            for n, ref in enumerate(ins):

                @pl.when(piece == n)
                def _():
                    for side in range(2):
                        cols = slice((side * kv_heads + h) * HEAD_DIM, (side * kv_heads + h + 1) * HEAD_DIM)
                        out_ref[o, :, cols] = ref[pl.ds(start, rows), cols]


def pick(kv_heads, rows, meta, pieces):
    width = pieces[0].shape[1]
    return pl.pallas_call(
        functools.partial(pick_kernel, kv_heads, pieces),
        out_shape=jax.ShapeDtypeStruct((2, rows, width), jnp.bfloat16),
        in_specs=[SMEM] + [VMEM] * len(pieces),
        out_specs=VMEM,
        compiler_params=pltpu.CompilerParams(vmem_limit_bytes=2 * 2**20),
        cost_estimate=pl.CostEstimate(flops=2**20, bytes_accessed=2**20, transcendentals=0),
        name="pick",
    )(meta, *pieces)


def pack_kernel(heads, m_ref, l_ref, out_ref):
    rows = out_ref.shape[0]
    lane = lax.broadcasted_iota(jnp.int32, out_ref.shape, 1)
    out = jnp.zeros(out_ref.shape, jnp.float32)
    for j in range(heads):
        at = slice(j * HEAD_DIM, (j + 1) * HEAD_DIM)
        out = jnp.where(lane == j, m_ref[rows:, at], out)
        out = jnp.where(lane == heads + j, l_ref[rows:, at], out)
    out_ref[...] = out


def merge_kernel(heads, m_ref, l_ref, acc_ref, stats_ref, other_ref, cache_ref, cache_other_ref, out_ref, cache_out):
    rows = out_ref.shape[0]
    scale = math.log2(math.e) / math.sqrt(HEAD_DIM)
    stats = stats_ref[...]
    for j in range(heads):
        at = slice(j * HEAD_DIM, (j + 1) * HEAD_DIM)
        m_b = stats[:, j : j + 1]
        l_b = stats[:, heads + j : heads + j + 1]
        m_a = m_ref[0:rows, at]
        m = jnp.maximum(m_a, m_b)
        fa = jnp.exp2((m_a - m) * scale)
        fb = jnp.exp2((m_b - m) * scale)
        total = l_ref[0:rows, at] * fa + l_b * fb
        out_ref[:, at] = ((acc_ref[0:rows, at] * fa + other_ref[:, at] * fb) / total).astype(out_ref.dtype)
    cache_out[...] = cache_ref[0] + cache_other_ref[...]


def local(queries, key_rows, value_rows, span_order, kept_blocks):
    n = lax.axis_size("seq")
    chips = n // 2
    me = lax.axis_index("seq")
    rows, width = queries.shape
    kv_heads = key_rows.shape[1] // HEAD_DIM
    group = width // key_rows.shape[1]
    heads = kv_heads * group
    pair = [(i, i ^ 1) for i in range(n)]
    rings = [
        {hop: [(i, ((i // 2 + (hop if i % 2 == t else -hop)) % chips) * 2 + 1 - i % 2) for i in range(n)] for hop in (1, 2)}
        for t in range(2)
    ]
    move = functools.partial(lax.ppermute, axis_name="seq")

    rounds = chips // 2
    cache_rows = kept_blocks.shape[1] * BLOCK // n
    own, kpos, qpos, meta = setup(kv_heads, chips, cache_rows, me, span_order, kept_blocks, key_rows, value_rows)
    partner = move(own, perm=pair)
    q_partner = move(queries, perm=pair)

    front, pieces, state = (own, partner), [own, partner], None
    for r in range(rounds // 2 + 1):
        arrived = {}
        if r < rounds // 2:
            for hop in (2, 1):
                for x in range(2):
                    arrived[hop, x] = move(front[x], perm=rings[r % 2][hop])
        else:
            cache = pick(kv_heads, cache_rows, meta, pieces)
            cache_other = move(cache[1], perm=pair)
        row = max(2 * r - 1, 0)
        state = attend(row, kv_heads, group, queries, q_partner, pieces[2 * row :], kpos, qpos, state)
        if arrived:
            front = (arrived[2, 0], arrived[2, 1])
            pieces += [arrived[hop, x] for hop in (1, 2) for x in range(2)]

    m, l, acc = state
    stats = pl.pallas_call(
        functools.partial(pack_kernel, heads),
        out_shape=jax.ShapeDtypeStruct((rows, HEAD_DIM), jnp.float32),
        in_specs=[VMEM] * 2,
        out_specs=VMEM,
        compiler_params=pltpu.CompilerParams(vmem_limit_bytes=8 * 2**20),
        name="pack",
    )(m, l)
    other = move(acc[rows:], perm=pair)
    stats_other = move(stats, perm=pair)
    return pl.pallas_call(
        functools.partial(merge_kernel, heads),
        out_shape=(
            jax.ShapeDtypeStruct((rows, width), jnp.bfloat16),
            jax.ShapeDtypeStruct((cache_rows, 2 * key_rows.shape[1]), jnp.bfloat16),
        ),
        in_specs=[VMEM] * 7,
        out_specs=(VMEM,) * 2,
        compiler_params=pltpu.CompilerParams(vmem_limit_bytes=16 * 2**20),
        name="merge",
    )(m, l, acc, stats_other, other, cache, cache_other)


def solution(mesh):
    placed = (
        P(("groups", "seq"), None),
        P(("groups", "seq"), None),
        P(("groups", "seq"), None),
        P("groups"),
        P("groups", None),
    )
    return jax.shard_map(
        local,
        mesh=mesh,
        in_specs=placed,
        out_specs=(P(("groups", "seq"), None), P(("groups", "seq"), None)),
        check_vma=False,
    )
```

```python
import functools
import math

import jax
import jax.numpy as jnp
from jax import lax
from jax.experimental import pallas as pl
from jax.experimental.pallas import tpu as pltpu
from jax.sharding import PartitionSpec as P


HEAD_DIM = 128
BLOCK = 512
LOW = -1e20
HIDDEN = -1e30
UNROLL = 7
SETUP_VMEM = 63 * 2**20
VMEM = pl.BlockSpec(memory_space=pltpu.VMEM)
SMEM = pl.BlockSpec(memory_space=pltpu.SMEM)


def attend_kernel(first, kv_heads, group, line, count, qo_ref, qp_ref, pos_ref, *refs):
    pieces, refs = refs[:count], refs[count:]
    if first:
        m_out, l_out, acc_out, bias, keys, values = refs
        m_in = l_in = acc_in = None
    else:
        m_in, l_in, acc_in, m_out, l_out, acc_out, bias, keys, values = refs
    rows = qo_ref.shape[0]
    piece = pieces[0].shape[0]
    scale = math.log2(math.e) / math.sqrt(HEAD_DIM)
    ones = jnp.ones((count * piece, HEAD_DIM), jnp.bfloat16)
    for n, ref in enumerate(pieces):
        part = slice(n * piece, (n + 1) * piece)
        kpos = pos_ref[line + n : line + n + 1, :]
        bias[:, part] = jnp.where(kpos <= pos_ref[pos_ref.shape[0] - 2 * rows :, :], 0.0, HIDDEN)
        for h in range(kv_heads):
            keys[h, part, :] = ref[:, h * HEAD_DIM : (h + 1) * HEAD_DIM]
            values[h, part, 0:HEAD_DIM] = ref[:, (kv_heads + h) * HEAD_DIM : (kv_heads + h + 1) * HEAD_DIM]
    for h in range(kv_heads):
        values[h, :, HEAD_DIM:] = ones

    def one_head(j):
        h = j // group
        at = pl.ds(pl.multiple_of(j * HEAD_DIM, HEAD_DIM), HEAD_DIM)
        q = jnp.concatenate([qo_ref[:, at], qp_ref[:, at]], axis=0)
        s = lax.dot_general(q, keys[h], (((1,), (1,)), ((), ())), preferred_element_type=jnp.float32)
        s = s + bias[...]
        top = jnp.max(s, axis=1, keepdims=True)
        if first:
            m_new = jnp.broadcast_to(jnp.maximum(top, LOW), (2 * rows, HEAD_DIM))
        else:
            m_old = m_in[:, at]
            m_new = jnp.maximum(m_old, top)
        shift = m_new * scale
        weights = jnp.exp2(s * scale - jnp.concatenate([shift] * count, axis=1)).astype(jnp.bfloat16)
        mixed = jnp.dot(weights, values[h], preferred_element_type=jnp.float32)
        m_out[:, at] = m_new
        if first:
            acc_out[:, at] = mixed[:, :HEAD_DIM]
            l_out[:, at] = mixed[:, HEAD_DIM:]
        else:
            factor = jnp.exp2((m_old - m_new) * scale)
            acc_out[:, at] = acc_in[:, at] * factor + mixed[:, :HEAD_DIM]
            l_out[:, at] = l_in[:, at] * factor + mixed[:, HEAD_DIM:]

    def some_heads(step, carry):
        for u in range(UNROLL):
            one_head(step * UNROLL + u)
        return carry

    lax.fori_loop(0, kv_heads * group // UNROLL, some_heads, 0)


def attend(line, kv_heads, group, qo, qp, pieces, pos, state):
    rows, width = qo.shape
    count, piece = len(pieces), pieces[0].shape[0]
    part = jax.ShapeDtypeStruct((2 * rows, width), jnp.float32)
    first = state is None
    args = (qo, qp, pos) + tuple(pieces) + (() if first else tuple(state))
    flops = 2 * 2 * 2 * rows * count * piece * width * 2
    return pl.pallas_call(
        functools.partial(attend_kernel, first, kv_heads, group, line, count),
        out_shape=(part, part, part),
        in_specs=[VMEM] * len(args),
        out_specs=(VMEM,) * 3,
        scratch_shapes=[
            pltpu.VMEM((2 * rows, count * piece), jnp.float32),
            pltpu.VMEM((kv_heads, count * piece, HEAD_DIM), jnp.bfloat16),
            pltpu.VMEM((kv_heads, count * piece, 2 * HEAD_DIM), jnp.bfloat16),
        ],
        input_output_aliases={} if first else {3 + count + i: i for i in range(3)},
        compiler_params=pltpu.CompilerParams(vmem_limit_bytes=8 * 2**20),
        cost_estimate=pl.CostEstimate(flops=flops, bytes_accessed=2**20, transcendentals=2**20),
        name="attend",
    )(*args)


def key_lines(chips):
    return -(-2 * (chips // 2 + 1) // 8) * 8


def moves_right(core, r):
    return lax.rem(core + r, 2)


def setup_kernel(kv_heads, chips, span, cache_rows, me_ref, order_hbm, row_hbm, kept_hbm, k_hbm, v_hbm, own_ref, pos_ref, meta_ref, order_ref, row_ref, kept_ref, sems):
    width = k_hbm.shape[1]
    copies = [
        pltpu.make_async_copy(order_hbm, order_ref, sems.at[0]),
        pltpu.make_async_copy(row_hbm, row_ref, sems.at[1]),
        pltpu.make_async_copy(kept_hbm, kept_ref, sems.at[2]),
        pltpu.make_async_copy(k_hbm, own_ref.at[:, :width], sems.at[3]),
        pltpu.make_async_copy(v_hbm, own_ref.at[:, width:], sems.at[4]),
    ]
    for copy in copies:
        copy.start()
    me = me_ref[0]
    chip, core = me // 2, lax.rem(me, 2)
    half = chips // 2
    lane = lax.broadcasted_iota(jnp.int32, (1, 2 * span), 1)
    line = lax.broadcasted_iota(jnp.int32, (span, HEAD_DIM), 0)
    lines = key_lines(chips)
    for copy in copies[:3]:
        copy.wait()
    for s in range(half + 1):
        r = (s - 1) // 2
        from_chip = chip if s == 0 else lax.rem(chip + s - 2 * s * moves_right(core, r) + chips, chips)
        first = core if s == 0 or r % 2 == 1 else 1 - core
        src = (2 * from_chip + first, 2 * from_chip + 1 - first)
        for x in range(2):
            low, high = order_ref[2 * src[x]] * span, (order_ref[2 * src[x] + 1] - 1) * span
            pos_ref[2 * s + x : 2 * s + x + 1, :] = lane + jnp.where(lane < span, low, high)
        if s == 0:
            for i in range(4):
                at = lines + i * span
                pos_ref[at : at + span, :] = line + order_ref[2 * src[i // 2] + i % 2] * span
    slots = lax.broadcasted_iota(jnp.int32, row_ref.shape, 1)
    for o in range(2):
        owner = me + o * (1 - 2 * core)
        first_row = owner * cache_rows
        for h in range(kv_heads):
            src = kept_ref[h, first_row // BLOCK] * BLOCK + lax.rem(first_row, BLOCK)
            slot = jnp.sum(jnp.where(row_ref[...] == src // span, slots, 0))
            dev = slot // 2
            back = lax.rem(chip - dev // 2 + chips, chips)
            right = jnp.where(back <= half, 1, 0)
            far = jnp.where(back <= half, back, chips - back)
            r = (far + 1) // 2 - 1
            same = (far == 0) | (lax.rem(r + 2, 2) == 1)
            first = jnp.where(same, core, 1 - core)
            side = jnp.where(lax.rem(dev, 2) == first, 0, 1)
            here = jnp.where(far == 0, side == 1, moves_right(core, r + 2) == right)
            here = jnp.where(far == half, side == 0, here)
            at = (o * kv_heads + h) * 2
            meta_ref[at] = jnp.where(here, 2 * far + side, -1)
            meta_ref[at + 1] = lax.rem(slot, 2) * span + lax.rem(src, span)
    for copy in copies[3:]:
        copy.wait()


def setup(kv_heads, chips, cache_rows, me, span_order, kept_blocks, key_rows, value_rows):
    rows, width = key_rows.shape
    return pl.pallas_call(
        functools.partial(setup_kernel, kv_heads, chips, rows // 2, cache_rows),
        out_shape=(
            jax.ShapeDtypeStruct((rows, 2 * width), jnp.bfloat16),
            jax.ShapeDtypeStruct((key_lines(chips) + 2 * rows, HEAD_DIM), jnp.int32),
            jax.ShapeDtypeStruct((4 * kv_heads,), jnp.int32),
        ),
        in_specs=[SMEM] + [pl.BlockSpec(memory_space=pltpu.HBM)] * 5,
        out_specs=(VMEM, VMEM, SMEM),
        scratch_shapes=[
            pltpu.SMEM(span_order.shape, jnp.int32),
            pltpu.VMEM((1,) + span_order.shape, jnp.int32),
            pltpu.SMEM(kept_blocks.shape, jnp.int32),
            pltpu.SemaphoreType.DMA((5,)),
        ],
        compiler_params=pltpu.CompilerParams(vmem_limit_bytes=SETUP_VMEM),
        name="setup",
    )(me.reshape(1), span_order, span_order.reshape(1, -1), kept_blocks, key_rows, value_rows)


def pick_kernel(kv_heads, pieces, meta_ref, *refs):
    ins, out_ref = refs[: len(pieces)], refs[len(pieces)]
    out_ref[...] = jnp.zeros_like(out_ref)
    owners = 2
    rows = out_ref.shape[1]
    for o in range(owners):
        for h in range(kv_heads):
            at = (o * kv_heads + h) * 2
            piece = meta_ref[at]
            start = pl.multiple_of(meta_ref[at + 1], 32)
            for low in range(0, len(ins), 6):

                @pl.when((piece >= low) & (piece < low + 6))
                def _():
                    for n in range(low, min(low + 6, len(ins))):

                        @pl.when(piece == n)
                        def _():
                            for side in range(2):
                                at = (side * kv_heads + h) * HEAD_DIM
                                cols = slice(at, at + HEAD_DIM)
                                out_ref[o, :, cols] = ins[n][pl.ds(start, rows), cols]


def pick(kv_heads, rows, meta, pieces):
    width = pieces[0].shape[1]
    return pl.pallas_call(
        functools.partial(pick_kernel, kv_heads, pieces),
        out_shape=jax.ShapeDtypeStruct((2, rows, width), jnp.bfloat16),
        in_specs=[SMEM] + [VMEM] * len(pieces),
        out_specs=VMEM,
        compiler_params=pltpu.CompilerParams(vmem_limit_bytes=2 * 2**20),
        cost_estimate=pl.CostEstimate(flops=2**20, bytes_accessed=2**20, transcendentals=0),
        name="pick",
    )(meta, *pieces)


def pack_kernel(heads, m_ref, l_ref, out_ref):
    rows = out_ref.shape[0]
    lane = lax.broadcasted_iota(jnp.int32, out_ref.shape, 1)
    out = jnp.zeros(out_ref.shape, jnp.float32)
    for j in range(heads):
        at = slice(j * HEAD_DIM, (j + 1) * HEAD_DIM)
        out = jnp.where(lane == j, m_ref[rows:, at], out)
        out = jnp.where(lane == heads + j, l_ref[rows:, at], out)
    out_ref[...] = out


def merge_kernel(heads, m_ref, l_ref, acc_ref, stats_ref, other_ref, cache_ref, cache_other_ref, out_ref, cache_out):
    rows = out_ref.shape[0]
    scale = math.log2(math.e) / math.sqrt(HEAD_DIM)
    stats = stats_ref[...]
    for j in range(heads):
        at = slice(j * HEAD_DIM, (j + 1) * HEAD_DIM)
        m_b = stats[:, j : j + 1]
        l_b = stats[:, heads + j : heads + j + 1]
        m_a = m_ref[0:rows, at]
        m = jnp.maximum(m_a, m_b)
        fa = jnp.exp2((m_a - m) * scale)
        fb = jnp.exp2((m_b - m) * scale)
        total = l_ref[0:rows, at] * fa + l_b * fb
        out_ref[:, at] = ((acc_ref[0:rows, at] * fa + other_ref[:, at] * fb) / total).astype(out_ref.dtype)
    cache_out[...] = cache_ref[0] + cache_other_ref[...]


def local(queries, key_rows, value_rows, span_order, kept_blocks):
    n = lax.axis_size("seq")
    chips = n // 2
    me = lax.axis_index("seq")
    rows, width = queries.shape
    kv_heads = key_rows.shape[1] // HEAD_DIM
    group = width // key_rows.shape[1]
    heads = kv_heads * group
    pair = [(i, i ^ 1) for i in range(n)]
    rings = [
        {hop: [(i, ((i // 2 + (hop if i % 2 == t else -hop)) % chips) * 2 + 1 - i % 2) for i in range(n)] for hop in (1, 2)}
        for t in range(2)
    ]
    move = functools.partial(lax.ppermute, axis_name="seq")

    rounds = chips // 2
    cache_rows = kept_blocks.shape[1] * BLOCK // n
    own, pos, meta = setup(kv_heads, chips, cache_rows, me, span_order, kept_blocks, key_rows, value_rows)
    partner = move(own, perm=pair)
    q_partner = move(queries, perm=pair)

    front, pieces, state = (own, partner), [own, partner], None
    for r in range(rounds // 2 + 1):
        arrived = {}
        if r < rounds // 2:
            for hop in (2, 1):
                for x in range(1 if hop == 2 and r == rounds // 2 - 1 else 2):
                    arrived[hop, x] = move(front[x], perm=rings[r % 2][hop])
        row = max(2 * r - 1, 0)
        now = pieces[2 * row :] if r else [partner]
        state = attend(2 * row if r else 1, kv_heads, group, queries, q_partner, now, pos, state)
        if arrived:
            front = (arrived[2, 0], arrived.get((2, 1)))
            pieces += [arrived[hop, x] for hop in (1, 2) for x in range(2) if (hop, x) in arrived]

    m, l, acc = state
    cache = pick(kv_heads, cache_rows, meta, [partner] + pieces[1:])
    cache_other = move(cache[1], perm=pair)
    stats = pl.pallas_call(
        functools.partial(pack_kernel, heads),
        out_shape=jax.ShapeDtypeStruct((rows, HEAD_DIM), jnp.float32),
        in_specs=[VMEM] * 2,
        out_specs=VMEM,
        compiler_params=pltpu.CompilerParams(vmem_limit_bytes=8 * 2**20),
        name="pack",
    )(m, l)
    other = move(acc[rows:], perm=pair)
    stats_other = move(stats, perm=pair)
    return pl.pallas_call(
        functools.partial(merge_kernel, heads),
        out_shape=(
            jax.ShapeDtypeStruct((rows, width), jnp.bfloat16),
            jax.ShapeDtypeStruct((cache_rows, 2 * key_rows.shape[1]), jnp.bfloat16),
        ),
        in_specs=[VMEM] * 7,
        out_specs=(VMEM,) * 2,
        compiler_params=pltpu.CompilerParams(vmem_limit_bytes=16 * 2**20),
        name="merge",
    )(m, l, acc, stats_other, other, cache, cache_other)


def solution(mesh):
    placed = (
        P(("groups", "seq"), None),
        P(("groups", "seq"), None),
        P(("groups", "seq"), None),
        P("groups"),
        P("groups", None),
    )
    return jax.shard_map(
        local,
        mesh=mesh,
        in_specs=placed,
        out_specs=(P(("groups", "seq"), None), P(("groups", "seq"), None)),
        check_vma=False,
    )
```

```python
import functools
import math

import jax
import jax.numpy as jnp
from jax import lax
from jax.experimental import pallas as pl
from jax.experimental.pallas import tpu as pltpu
from jax.sharding import PartitionSpec as P


HEAD_DIM = 128
BLOCK = 512
LOW = -1e20
HIDDEN = -1e30
UNROLL = 7
SETUP_VMEM = 63 * 2**20
VMEM = pl.BlockSpec(memory_space=pltpu.VMEM)
SMEM = pl.BlockSpec(memory_space=pltpu.SMEM)


def attend_kernel(first, kv_heads, group, lines, q_ref, pos_ref, *refs):
    count = len(lines)
    pieces, refs = refs[:count], refs[count:]
    if first:
        m_out, l_out, acc_out, bias, keys, values = refs
        m_in = l_in = acc_in = None
    else:
        m_in, l_in, acc_in, m_out, l_out, acc_out, bias, keys, values = refs
    rows = q_ref.shape[0]
    piece = pieces[0].shape[0]
    scale = math.log2(math.e) / math.sqrt(HEAD_DIM)
    ones = jnp.ones((count * piece, HEAD_DIM), jnp.bfloat16)
    for n, ref in enumerate(pieces):
        part = slice(n * piece, (n + 1) * piece)
        kpos = pos_ref[lines[n] : lines[n] + 1, :]
        bias[:, part] = jnp.where(kpos <= pos_ref[pos_ref.shape[0] - rows :, :], 0.0, HIDDEN)
        for h in range(kv_heads):
            keys[h, part, :] = ref[:, h * HEAD_DIM : (h + 1) * HEAD_DIM]
            values[h, part, 0:HEAD_DIM] = ref[:, (kv_heads + h) * HEAD_DIM : (kv_heads + h + 1) * HEAD_DIM]
    for h in range(kv_heads):
        values[h, :, HEAD_DIM:] = ones

    def one_head(j):
        h = j // group
        at = pl.ds(pl.multiple_of(j * HEAD_DIM, HEAD_DIM), HEAD_DIM)
        s = lax.dot_general(q_ref[:, at], keys[h], (((1,), (1,)), ((), ())), preferred_element_type=jnp.float32)
        s = s + bias[...]
        top = jnp.max(s, axis=1, keepdims=True)
        if first:
            m_new = jnp.broadcast_to(jnp.maximum(top, LOW), (rows, HEAD_DIM))
        else:
            m_old = m_in[:, at]
            m_new = jnp.maximum(m_old, top)
        shift = m_new * scale
        weights = jnp.exp2(s * scale - jnp.concatenate([shift] * count, axis=1)).astype(jnp.bfloat16)
        mixed = jnp.dot(weights, values[h], preferred_element_type=jnp.float32)
        m_out[:, at] = m_new
        if first:
            acc_out[:, at] = mixed[:, :HEAD_DIM]
            l_out[:, at] = mixed[:, HEAD_DIM:]
        else:
            factor = jnp.exp2((m_old - m_new) * scale)
            acc_out[:, at] = acc_in[:, at] * factor + mixed[:, :HEAD_DIM]
            l_out[:, at] = l_in[:, at] * factor + mixed[:, HEAD_DIM:]

    def some_heads(step, carry):
        for u in range(UNROLL):
            one_head(step * UNROLL + u)
        return carry

    lax.fori_loop(0, kv_heads * group // UNROLL, some_heads, 0)


def attend(lines, kv_heads, group, q, pieces, pos, state):
    rows, width = q.shape
    count, piece = len(pieces), pieces[0].shape[0]
    part = jax.ShapeDtypeStruct((rows, width), jnp.float32)
    first = state is None
    args = (q, pos) + tuple(pieces) + (() if first else tuple(state))
    flops = 2 * 2 * rows * count * piece * width * 2
    return pl.pallas_call(
        functools.partial(attend_kernel, first, kv_heads, group, lines),
        out_shape=(part, part, part),
        in_specs=[VMEM] * len(args),
        out_specs=(VMEM,) * 3,
        scratch_shapes=[
            pltpu.VMEM((rows, count * piece), jnp.float32),
            pltpu.VMEM((kv_heads, count * piece, HEAD_DIM), jnp.bfloat16),
            pltpu.VMEM((kv_heads, count * piece, 2 * HEAD_DIM), jnp.bfloat16),
        ],
        input_output_aliases={} if first else {2 + count + i: i for i in range(3)},
        compiler_params=pltpu.CompilerParams(vmem_limit_bytes=8 * 2**20),
        cost_estimate=pl.CostEstimate(flops=flops, bytes_accessed=2**20, transcendentals=2**20),
        name="attend",
    )(*args)


def gather_kernel(own_ref, partner_ref, pos_ref, q_out, pos_out):
    rows = own_ref.shape[0]
    q_out[:rows, :] = own_ref[...]
    q_out[rows:, :] = partner_ref[...]
    pos_out[...] = pos_ref[...]


def gather(own, partner, pos):
    rows, width = own.shape
    return pl.pallas_call(
        gather_kernel,
        out_shape=(jax.ShapeDtypeStruct((2 * rows, width), own.dtype), jax.ShapeDtypeStruct(pos.shape, pos.dtype)),
        in_specs=[VMEM] * 3,
        out_specs=(VMEM,) * 2,
        compiler_params=pltpu.CompilerParams(vmem_limit_bytes=4 * 2**20),
        cost_estimate=pl.CostEstimate(flops=2**24, bytes_accessed=2**20, transcendentals=0),
        name="gather",
    )(own, partner, pos)


def key_lines(chips):
    return -(-2 * (chips // 2 + 1) // 8) * 8


def moves_right(core, r):
    return lax.rem(core + r, 2)


def setup_kernel(kv_heads, chips, span, cache_rows, me_ref, order_hbm, row_hbm, kept_hbm, k_hbm, v_hbm, own_ref, pos_ref, meta_ref, order_ref, row_ref, kept_ref, sems):
    width = k_hbm.shape[1]
    copies = [
        pltpu.make_async_copy(order_hbm, order_ref, sems.at[0]),
        pltpu.make_async_copy(row_hbm, row_ref, sems.at[1]),
        pltpu.make_async_copy(kept_hbm, kept_ref, sems.at[2]),
        pltpu.make_async_copy(k_hbm, own_ref.at[:, :width], sems.at[3]),
        pltpu.make_async_copy(v_hbm, own_ref.at[:, width:], sems.at[4]),
    ]
    for copy in copies:
        copy.start()
    me = me_ref[0]
    chip, core = me // 2, lax.rem(me, 2)
    half = chips // 2
    lane = lax.broadcasted_iota(jnp.int32, (1, 2 * span), 1)
    line = lax.broadcasted_iota(jnp.int32, (span, HEAD_DIM), 0)
    lines = key_lines(chips)
    for copy in copies[:3]:
        copy.wait()
    for s in range(half + 1):
        r = (s - 1) // 2
        from_chip = chip if s == 0 else lax.rem(chip + s - 2 * s * moves_right(core, r) + chips, chips)
        first = core if s == 0 or r % 2 == 1 else 1 - core
        src = (2 * from_chip + first, 2 * from_chip + 1 - first)
        for x in range(2):
            low, high = order_ref[2 * src[x]] * span, (order_ref[2 * src[x] + 1] - 1) * span
            pos_ref[2 * s + x : 2 * s + x + 1, :] = lane + jnp.where(lane < span, low, high)
        if s == 0:
            for i in range(4):
                at = lines + i * span
                pos_ref[at : at + span, :] = line + order_ref[2 * src[i // 2] + i % 2] * span
    slots = lax.broadcasted_iota(jnp.int32, row_ref.shape, 1)
    for o in range(2):
        owner = me + o * (1 - 2 * core)
        first_row = owner * cache_rows
        for h in range(kv_heads):
            src = kept_ref[h, first_row // BLOCK] * BLOCK + lax.rem(first_row, BLOCK)
            slot = jnp.sum(jnp.where(row_ref[...] == src // span, slots, 0))
            dev = slot // 2
            back = lax.rem(chip - dev // 2 + chips, chips)
            right = jnp.where(back <= half, 1, 0)
            far = jnp.where(back <= half, back, chips - back)
            r = (far + 1) // 2 - 1
            same = (far == 0) | (lax.rem(r + 2, 2) == 1)
            first = jnp.where(same, core, 1 - core)
            side = jnp.where(lax.rem(dev, 2) == first, 0, 1)
            here = jnp.where(far == 0, side == 1, moves_right(core, r + 2) == right)
            here = jnp.where(far == half, side == 0, here)
            at = (o * kv_heads + h) * 2
            meta_ref[at] = jnp.where(here, 2 * far + side, -1)
            meta_ref[at + 1] = lax.rem(slot, 2) * span + lax.rem(src, span)
    for copy in copies[3:]:
        copy.wait()


def setup(kv_heads, chips, cache_rows, me, span_order, kept_blocks, key_rows, value_rows):
    rows, width = key_rows.shape
    return pl.pallas_call(
        functools.partial(setup_kernel, kv_heads, chips, rows // 2, cache_rows),
        out_shape=(
            jax.ShapeDtypeStruct((rows, 2 * width), jnp.bfloat16),
            jax.ShapeDtypeStruct((key_lines(chips) + 2 * rows, HEAD_DIM), jnp.int32),
            jax.ShapeDtypeStruct((4 * kv_heads,), jnp.int32),
        ),
        in_specs=[SMEM] + [pl.BlockSpec(memory_space=pltpu.HBM)] * 5,
        out_specs=(VMEM, VMEM, SMEM),
        scratch_shapes=[
            pltpu.SMEM(span_order.shape, jnp.int32),
            pltpu.VMEM((1,) + span_order.shape, jnp.int32),
            pltpu.SMEM(kept_blocks.shape, jnp.int32),
            pltpu.SemaphoreType.DMA((5,)),
        ],
        compiler_params=pltpu.CompilerParams(vmem_limit_bytes=SETUP_VMEM),
        name="setup",
    )(me.reshape(1), span_order, span_order.reshape(1, -1), kept_blocks, key_rows, value_rows)


def pick_kernel(kv_heads, pieces, meta_ref, *refs):
    ins, out_ref = refs[: len(pieces)], refs[len(pieces)]
    out_ref[...] = jnp.zeros_like(out_ref)
    owners = 2
    rows = out_ref.shape[1]
    for o in range(owners):
        for h in range(kv_heads):
            at = (o * kv_heads + h) * 2
            piece = meta_ref[at]
            start = pl.multiple_of(meta_ref[at + 1], 32)
            for low in range(0, len(ins), 6):

                @pl.when((piece >= low) & (piece < low + 6))
                def _():
                    for n in range(low, min(low + 6, len(ins))):

                        @pl.when(piece == n)
                        def _():
                            for side in range(2):
                                at = (side * kv_heads + h) * HEAD_DIM
                                cols = slice(at, at + HEAD_DIM)
                                out_ref[o, :, cols] = ins[n][pl.ds(start, rows), cols]


def pick(kv_heads, rows, meta, pieces):
    width = pieces[0].shape[1]
    return pl.pallas_call(
        functools.partial(pick_kernel, kv_heads, pieces),
        out_shape=jax.ShapeDtypeStruct((2, rows, width), jnp.bfloat16),
        in_specs=[SMEM] + [VMEM] * len(pieces),
        out_specs=VMEM,
        compiler_params=pltpu.CompilerParams(vmem_limit_bytes=2 * 2**20),
        cost_estimate=pl.CostEstimate(flops=2**20, bytes_accessed=2**20, transcendentals=0),
        name="pick",
    )(meta, *pieces)


def pack_kernel(heads, m_ref, l_ref, out_ref):
    rows = out_ref.shape[0]
    lane = lax.broadcasted_iota(jnp.int32, out_ref.shape, 1)
    out = jnp.zeros(out_ref.shape, jnp.float32)
    for j in range(heads):
        at = slice(j * HEAD_DIM, (j + 1) * HEAD_DIM)
        out = jnp.where(lane == j, m_ref[rows:, at], out)
        out = jnp.where(lane == heads + j, l_ref[rows:, at], out)
    out_ref[...] = out


def merge_kernel(heads, m_ref, l_ref, acc_ref, stats_ref, other_ref, cache_ref, cache_other_ref, out_ref, cache_out):
    rows = out_ref.shape[0]
    scale = math.log2(math.e) / math.sqrt(HEAD_DIM)
    stats = stats_ref[...]
    for j in range(heads):
        at = slice(j * HEAD_DIM, (j + 1) * HEAD_DIM)
        m_b = stats[:, j : j + 1]
        l_b = stats[:, heads + j : heads + j + 1]
        m_a = m_ref[0:rows, at]
        m = jnp.maximum(m_a, m_b)
        fa = jnp.exp2((m_a - m) * scale)
        fb = jnp.exp2((m_b - m) * scale)
        total = l_ref[0:rows, at] * fa + l_b * fb
        out_ref[:, at] = ((acc_ref[0:rows, at] * fa + other_ref[:, at] * fb) / total).astype(out_ref.dtype)
    cache_out[...] = cache_ref[0] + cache_other_ref[...]


def local(queries, key_rows, value_rows, span_order, kept_blocks):
    n = lax.axis_size("seq")
    chips = n // 2
    me = lax.axis_index("seq")
    rows, width = queries.shape
    kv_heads = key_rows.shape[1] // HEAD_DIM
    group = width // key_rows.shape[1]
    heads = kv_heads * group
    pair = [(i, i ^ 1) for i in range(n)]
    rings = [
        {hop: [(i, ((i // 2 + (hop if i % 2 == t else -hop)) % chips) * 2 + 1 - i % 2) for i in range(n)] for hop in (1, 2)}
        for t in range(2)
    ]
    move = functools.partial(lax.ppermute, axis_name="seq")

    rounds = chips // 2
    cache_rows = kept_blocks.shape[1] * BLOCK // n
    own, pos, meta = setup(kv_heads, chips, cache_rows, me, span_order, kept_blocks, key_rows, value_rows)
    partner = move(own, perm=pair)
    q_partner = move(queries, perm=pair)

    front, pieces, state = (own, partner), [own, partner], None
    for r in range(rounds // 2 + 1):
        arrived = {}
        if r < rounds // 2:
            for hop in (2, 1):
                for x in range(1 if hop == 2 and r == rounds // 2 - 1 else 2):
                    arrived[hop, x] = move(front[x], perm=rings[r % 2][hop])
        if r == 0:
            q, pos = gather(queries, q_partner, pos)
        else:
            at = 2 * (2 * r - 1)
            lines, now = tuple(range(at, len(pieces))), pieces[at:]
            if not arrived:
                lines, now = lines + (1,), now + [partner]
            state = attend(lines, kv_heads, group, q, now, pos, state)
        if arrived:
            front = (arrived[2, 0], arrived.get((2, 1)))
            pieces += [arrived[hop, x] for hop in (1, 2) for x in range(2) if (hop, x) in arrived]

    m, l, acc = state
    cache = pick(kv_heads, cache_rows, meta, [partner] + pieces[1:])
    cache_other = move(cache[1], perm=pair)
    stats = pl.pallas_call(
        functools.partial(pack_kernel, heads),
        out_shape=jax.ShapeDtypeStruct((rows, HEAD_DIM), jnp.float32),
        in_specs=[VMEM] * 2,
        out_specs=VMEM,
        compiler_params=pltpu.CompilerParams(vmem_limit_bytes=8 * 2**20),
        name="pack",
    )(m, l)
    other = move(acc[rows:], perm=pair)
    stats_other = move(stats, perm=pair)
    return pl.pallas_call(
        functools.partial(merge_kernel, heads),
        out_shape=(
            jax.ShapeDtypeStruct((rows, width), jnp.bfloat16),
            jax.ShapeDtypeStruct((cache_rows, 2 * key_rows.shape[1]), jnp.bfloat16),
        ),
        in_specs=[VMEM] * 7,
        out_specs=(VMEM,) * 2,
        compiler_params=pltpu.CompilerParams(vmem_limit_bytes=16 * 2**20),
        name="merge",
    )(m, l, acc, stats_other, other, cache, cache_other)


def solution(mesh):
    placed = (
        P(("groups", "seq"), None),
        P(("groups", "seq"), None),
        P(("groups", "seq"), None),
        P("groups"),
        P("groups", None),
    )
    return jax.shard_map(
        local,
        mesh=mesh,
        in_specs=placed,
        out_specs=(P(("groups", "seq"), None), P(("groups", "seq"), None)),
        check_vma=False,
    )
```

```python
import functools
import math

import jax
import jax.numpy as jnp
from jax import lax
from jax.experimental import pallas as pl
from jax.experimental.pallas import tpu as pltpu
from jax.sharding import PartitionSpec as P


HEAD_DIM = 128
BLOCK = 512
LOW = -1e20
HIDDEN = -1e30
UNROLL = 7
SETUP_VMEM = 63 * 2**20
VMEM = pl.BlockSpec(memory_space=pltpu.VMEM)
SMEM = pl.BlockSpec(memory_space=pltpu.SMEM)


def attend_kernel(first, kv_heads, group, line, count, qo_ref, qp_ref, pos_ref, *refs):
    piece, pieces, inputs = HEAD_DIM, [], 0
    while len(pieces) < count:
        ref, inputs = refs[inputs], inputs + 1
        pieces += [ref.at[at : at + piece] for at in range(0, ref.shape[0], piece)]
    refs = refs[inputs:]
    if first:
        m_out, l_out, acc_out, bias, keys, values = refs
        m_in = l_in = acc_in = None
    else:
        m_in, l_in, acc_in, m_out, l_out, acc_out, bias, keys, values = refs
    rows = qo_ref.shape[0]
    scale = math.log2(math.e) / math.sqrt(HEAD_DIM)
    ones = jnp.ones((count * piece, HEAD_DIM), jnp.bfloat16)
    for n, ref in enumerate(pieces):
        part = slice(n * piece, (n + 1) * piece)
        kpos = pos_ref[line + n : line + n + 1, :]
        bias[:, part] = jnp.where(kpos <= pos_ref[pos_ref.shape[0] - 2 * rows :, :], 0.0, HIDDEN)
        for h in range(kv_heads):
            keys[h, part, :] = ref[:, h * HEAD_DIM : (h + 1) * HEAD_DIM]
            values[h, part, 0:HEAD_DIM] = ref[:, (kv_heads + h) * HEAD_DIM : (kv_heads + h + 1) * HEAD_DIM]
    for h in range(kv_heads):
        values[h, :, HEAD_DIM:] = ones

    def one_head(j):
        h = j // group
        at = pl.ds(pl.multiple_of(j * HEAD_DIM, HEAD_DIM), HEAD_DIM)
        q = jnp.concatenate([qo_ref[:, at], qp_ref[:, at]], axis=0)
        s = lax.dot_general(q, keys[h], (((1,), (1,)), ((), ())), preferred_element_type=jnp.float32)
        s = s + bias[...]
        top = jnp.max(s, axis=1, keepdims=True)
        if first:
            m_new = jnp.broadcast_to(jnp.maximum(top, LOW), (2 * rows, HEAD_DIM))
        else:
            m_old = m_in[:, at]
            m_new = jnp.maximum(m_old, top)
        shift = m_new * scale
        weights = jnp.exp2(s * scale - jnp.concatenate([shift] * count, axis=1)).astype(jnp.bfloat16)
        mixed = jnp.dot(weights, values[h], preferred_element_type=jnp.float32)
        m_out[:, at] = m_new
        if first:
            acc_out[:, at] = mixed[:, :HEAD_DIM]
            l_out[:, at] = mixed[:, HEAD_DIM:]
        else:
            factor = jnp.exp2((m_old - m_new) * scale)
            acc_out[:, at] = acc_in[:, at] * factor + mixed[:, :HEAD_DIM]
            l_out[:, at] = l_in[:, at] * factor + mixed[:, HEAD_DIM:]

    def some_heads(step, carry):
        for u in range(UNROLL):
            one_head(step * UNROLL + u)
        return carry

    lax.fori_loop(0, kv_heads * group // UNROLL, some_heads, 0)


def attend(line, kv_heads, group, qo, qp, pieces, pos, state):
    rows, width = qo.shape
    piece = HEAD_DIM
    count = sum(x.shape[0] for x in pieces) // piece
    part = jax.ShapeDtypeStruct((2 * rows, width), jnp.float32)
    first = state is None
    args = (qo, qp, pos) + tuple(pieces) + (() if first else tuple(state))
    flops = 2 * 2 * 2 * rows * count * piece * width * 2
    return pl.pallas_call(
        functools.partial(attend_kernel, first, kv_heads, group, line, count),
        out_shape=(part, part, part),
        in_specs=[VMEM] * len(args),
        out_specs=(VMEM,) * 3,
        scratch_shapes=[
            pltpu.VMEM((2 * rows, count * piece), jnp.float32),
            pltpu.VMEM((kv_heads, count * piece, HEAD_DIM), jnp.bfloat16),
            pltpu.VMEM((kv_heads, count * piece, 2 * HEAD_DIM), jnp.bfloat16),
        ],
        input_output_aliases={} if first else {3 + len(pieces) + i: i for i in range(3)},
        compiler_params=pltpu.CompilerParams(vmem_limit_bytes=8 * 2**20),
        cost_estimate=pl.CostEstimate(flops=flops, bytes_accessed=2**20, transcendentals=2**20),
        name="attend",
    )(*args)


def join_kernel(a_ref, b_ref, out_ref):
    rows = a_ref.shape[0]
    out_ref[:rows, :] = a_ref[...]
    out_ref[rows:, :] = b_ref[...]


def join(a, b):
    return pl.pallas_call(
        join_kernel,
        out_shape=jax.ShapeDtypeStruct((2 * a.shape[0], a.shape[1]), a.dtype),
        in_specs=[VMEM] * 2,
        out_specs=VMEM,
        compiler_params=pltpu.CompilerParams(vmem_limit_bytes=2 * 2**20),
        cost_estimate=pl.CostEstimate(flops=2**20, bytes_accessed=2**19, transcendentals=0),
        name="join",
    )(a, b)


def key_lines(chips):
    return -(-2 * (chips // 2 + 1) // 8) * 8


def moves_right(core, r):
    return lax.rem(core + r, 2)


def setup_kernel(kv_heads, chips, span, cache_rows, me_ref, order_hbm, row_hbm, kept_hbm, k_hbm, v_hbm, own_ref, pos_ref, meta_ref, order_ref, row_ref, kept_ref, sems):
    width = k_hbm.shape[1]
    copies = [
        pltpu.make_async_copy(order_hbm, order_ref, sems.at[0]),
        pltpu.make_async_copy(row_hbm, row_ref, sems.at[1]),
        pltpu.make_async_copy(kept_hbm, kept_ref, sems.at[2]),
        pltpu.make_async_copy(k_hbm, own_ref.at[:, :width], sems.at[3]),
        pltpu.make_async_copy(v_hbm, own_ref.at[:, width:], sems.at[4]),
    ]
    for copy in copies:
        copy.start()
    me = me_ref[0]
    chip, core = me // 2, lax.rem(me, 2)
    half = chips // 2
    lane = lax.broadcasted_iota(jnp.int32, (1, 2 * span), 1)
    line = lax.broadcasted_iota(jnp.int32, (span, HEAD_DIM), 0)
    lines = key_lines(chips)
    for copy in copies[:3]:
        copy.wait()
    for s in range(half + 1):
        r = (s - 1) // 2
        from_chip = chip if s == 0 else lax.rem(chip + s - 2 * s * moves_right(core, r) + chips, chips)
        first = core if s == 0 or r % 2 == 1 else 1 - core
        src = (2 * from_chip + first, 2 * from_chip + 1 - first)
        for x in range(2):
            low, high = order_ref[2 * src[x]] * span, (order_ref[2 * src[x] + 1] - 1) * span
            pos_ref[2 * s + x : 2 * s + x + 1, :] = lane + jnp.where(lane < span, low, high)
        if s == 0:
            for i in range(4):
                at = lines + i * span
                pos_ref[at : at + span, :] = line + order_ref[2 * src[i // 2] + i % 2] * span
    slots = lax.broadcasted_iota(jnp.int32, row_ref.shape, 1)
    for o in range(2):
        owner = me + o * (1 - 2 * core)
        first_row = owner * cache_rows
        for h in range(kv_heads):
            src = kept_ref[h, first_row // BLOCK] * BLOCK + lax.rem(first_row, BLOCK)
            slot = jnp.sum(jnp.where(row_ref[...] == src // span, slots, 0))
            dev = slot // 2
            back = lax.rem(chip - dev // 2 + chips, chips)
            right = jnp.where(back <= half, 1, 0)
            far = jnp.where(back <= half, back, chips - back)
            r = (far + 1) // 2 - 1
            same = (far == 0) | (lax.rem(r + 2, 2) == 1)
            first = jnp.where(same, core, 1 - core)
            side = jnp.where(lax.rem(dev, 2) == first, 0, 1)
            here = jnp.where(far == 0, side == 1, moves_right(core, r + 2) == right)
            here = jnp.where(far == half, side == 0, here)
            at = (o * kv_heads + h) * 2
            meta_ref[at] = jnp.where(here, 2 * far + side, -1)
            meta_ref[at + 1] = lax.rem(slot, 2) * span + lax.rem(src, span)
    for copy in copies[3:]:
        copy.wait()


def setup(kv_heads, chips, cache_rows, me, span_order, kept_blocks, key_rows, value_rows):
    rows, width = key_rows.shape
    return pl.pallas_call(
        functools.partial(setup_kernel, kv_heads, chips, rows // 2, cache_rows),
        out_shape=(
            jax.ShapeDtypeStruct((rows, 2 * width), jnp.bfloat16),
            jax.ShapeDtypeStruct((key_lines(chips) + 2 * rows, HEAD_DIM), jnp.int32),
            jax.ShapeDtypeStruct((4 * kv_heads,), jnp.int32),
        ),
        in_specs=[SMEM] + [pl.BlockSpec(memory_space=pltpu.HBM)] * 5,
        out_specs=(VMEM, VMEM, SMEM),
        scratch_shapes=[
            pltpu.SMEM(span_order.shape, jnp.int32),
            pltpu.VMEM((1,) + span_order.shape, jnp.int32),
            pltpu.SMEM(kept_blocks.shape, jnp.int32),
            pltpu.SemaphoreType.DMA((5,)),
        ],
        compiler_params=pltpu.CompilerParams(vmem_limit_bytes=SETUP_VMEM),
        name="setup",
    )(me.reshape(1), span_order, span_order.reshape(1, -1), kept_blocks, key_rows, value_rows)


def pick_kernel(kv_heads, pieces, meta_ref, *refs):
    ins, out_ref = [], refs[len(pieces)]
    for ref in refs[: len(pieces)]:
        ins += [ref.at[at : at + HEAD_DIM] for at in range(0, ref.shape[0], HEAD_DIM)]
    out_ref[...] = jnp.zeros_like(out_ref)
    owners = 2
    rows = out_ref.shape[1]
    for o in range(owners):
        for h in range(kv_heads):
            at = (o * kv_heads + h) * 2
            piece = meta_ref[at]
            start = pl.multiple_of(meta_ref[at + 1], 32)
            for low in range(0, len(ins), 6):

                @pl.when((piece >= low) & (piece < low + 6))
                def _():
                    for n in range(low, min(low + 6, len(ins))):

                        @pl.when(piece == n)
                        def _():
                            for side in range(2):
                                at = (side * kv_heads + h) * HEAD_DIM
                                cols = slice(at, at + HEAD_DIM)
                                out_ref[o, :, cols] = ins[n][pl.ds(start, rows), cols]


def pick(kv_heads, rows, meta, pieces):
    width = pieces[0].shape[1]
    return pl.pallas_call(
        functools.partial(pick_kernel, kv_heads, pieces),
        out_shape=jax.ShapeDtypeStruct((2, rows, width), jnp.bfloat16),
        in_specs=[SMEM] + [VMEM] * len(pieces),
        out_specs=VMEM,
        compiler_params=pltpu.CompilerParams(vmem_limit_bytes=2 * 2**20),
        cost_estimate=pl.CostEstimate(flops=2**20, bytes_accessed=2**20, transcendentals=0),
        name="pick",
    )(meta, *pieces)


def pack_kernel(heads, m_ref, l_ref, out_ref):
    rows = out_ref.shape[0]
    lane = lax.broadcasted_iota(jnp.int32, out_ref.shape, 1)
    out = jnp.zeros(out_ref.shape, jnp.float32)
    for j in range(heads):
        at = slice(j * HEAD_DIM, (j + 1) * HEAD_DIM)
        out = jnp.where(lane == j, m_ref[rows:, at], out)
        out = jnp.where(lane == heads + j, l_ref[rows:, at], out)
    out_ref[...] = out


def merge_kernel(heads, m_ref, l_ref, acc_ref, stats_ref, other_ref, cache_ref, cache_other_ref, out_ref, cache_out):
    rows = out_ref.shape[0]
    scale = math.log2(math.e) / math.sqrt(HEAD_DIM)
    stats = stats_ref[...]
    for j in range(heads):
        at = slice(j * HEAD_DIM, (j + 1) * HEAD_DIM)
        m_b = stats[:, j : j + 1]
        l_b = stats[:, heads + j : heads + j + 1]
        m_a = m_ref[0:rows, at]
        m = jnp.maximum(m_a, m_b)
        fa = jnp.exp2((m_a - m) * scale)
        fb = jnp.exp2((m_b - m) * scale)
        total = l_ref[0:rows, at] * fa + l_b * fb
        out_ref[:, at] = ((acc_ref[0:rows, at] * fa + other_ref[:, at] * fb) / total).astype(out_ref.dtype)
    cache_out[...] = cache_ref[0] + cache_other_ref[...]


def local(queries, key_rows, value_rows, span_order, kept_blocks):
    n = lax.axis_size("seq")
    chips = n // 2
    me = lax.axis_index("seq")
    rows, width = queries.shape
    kv_heads = key_rows.shape[1] // HEAD_DIM
    group = width // key_rows.shape[1]
    heads = kv_heads * group
    pair = [(i, i ^ 1) for i in range(n)]
    rings = [
        {hop: [(i, ((i // 2 + (hop if i % 2 == t else -hop)) % chips) * 2 + 1 - i % 2) for i in range(n)] for hop in (1, 2)}
        for t in range(2)
    ]
    move = functools.partial(lax.ppermute, axis_name="seq")

    rounds = chips // 2
    cache_rows = kept_blocks.shape[1] * BLOCK // n
    own, pos, meta = setup(kv_heads, chips, cache_rows, me, span_order, kept_blocks, key_rows, value_rows)
    partner = move(own, perm=pair)
    q_partner = move(queries, perm=pair)

    front, pieces, now, state = [own, partner], [partner, partner], [partner], None
    for r in range(rounds // 2 + 1):
        far = []
        if r < rounds // 2:
            for x in range(1 if r == rounds // 2 - 1 else 2):
                far.append(move(front[x], perm=rings[r % 2][2]))
            both = join(*front)
            near = move(both, perm=rings[r % 2][1])
        state = attend(4 * r - 2 if r else 1, kv_heads, group, queries, q_partner, now, pos, state)
        if far:
            front, now = far, [near] + far
            pieces += now

    m, l, acc = state
    cache = pick(kv_heads, cache_rows, meta, pieces)
    cache_other = move(cache[1], perm=pair)
    stats = pl.pallas_call(
        functools.partial(pack_kernel, heads),
        out_shape=jax.ShapeDtypeStruct((rows, HEAD_DIM), jnp.float32),
        in_specs=[VMEM] * 2,
        out_specs=VMEM,
        compiler_params=pltpu.CompilerParams(vmem_limit_bytes=8 * 2**20),
        name="pack",
    )(m, l)
    other = move(acc[rows:], perm=pair)
    stats_other = move(stats, perm=pair)
    return pl.pallas_call(
        functools.partial(merge_kernel, heads),
        out_shape=(
            jax.ShapeDtypeStruct((rows, width), jnp.bfloat16),
            jax.ShapeDtypeStruct((cache_rows, 2 * key_rows.shape[1]), jnp.bfloat16),
        ),
        in_specs=[VMEM] * 7,
        out_specs=(VMEM,) * 2,
        compiler_params=pltpu.CompilerParams(vmem_limit_bytes=16 * 2**20),
        name="merge",
    )(m, l, acc, stats_other, other, cache, cache_other)


def solution(mesh):
    placed = (
        P(("groups", "seq"), None),
        P(("groups", "seq"), None),
        P(("groups", "seq"), None),
        P("groups"),
        P("groups", None),
    )
    return jax.shard_map(
        local,
        mesh=mesh,
        in_specs=placed,
        out_specs=(P(("groups", "seq"), None), P(("groups", "seq"), None)),
        check_vma=False,
    )
```
